32 devices in a mesh: chain: 16 (over z, x, core), shard: 2 (over y).
Axes of the slice: x: 2, y: 2, z: 4, core: 2. Of those that a mesh axis runs over, the one named last changes fastest.
Arguments:
- w_pair: bfloat16 [16, 2, 256, 4096], P('chain', None, 'shard'), may hold values from -6 to 6
- w_down: bfloat16 [16, 256, 4096], P('chain', 'shard'), may hold values from -6 to 6
- tokens: bfloat16 [16, 512, 4096], P('chain', 'shard'), may hold values from -6 to 6
- cotangent: bfloat16 [16, 512, 4096], P('chain', 'shard'), may hold values from -6 to 6
- seq_ids: int32 [16, 512], P('chain', 'shard'), may hold values from 0 to 7, never falling along the last dimension, each value on 1 to 128 neighbouring positions
- msg_left: bfloat16 [16, 2, 256, 4096], P('chain', None, 'shard'), may hold values from -9 to 9
- msg_right: bfloat16 [16, 2, 256, 4096], P('chain', None, 'shard'), may hold values from -9 to 9
- count_left: int32 [16], P('chain'), may hold values from 0 to 5, as said below
- count_right: int32 [16], P('chain'), may hold values from 0 to 5, as said below
Outputs:
- new_pair: bfloat16 [16, 2, 256, 4096], P('chain', None, 'shard')
The draws below stay inside these ranges and needn't reach their ends.
Inputs may be any that keep to these rules, and one draw needn't show every extreme that they name: count_left of worker w is at most min(w, 5); some worker at least 5 from both ends of the chain has count_left equal to 5. count_right of worker w is at most min(15 - w, 5); the same worker has count_right equal to 5.
All inputs are finite; a program needn't handle non-finite values.
Results may differ from the reference program's by a relative error of at most 0.0053.
Values may be sent and summed in bfloat16 or wider, within the bound.
No kernel may reach another device: no remote copies, remote signals or barrier semaphores. Data moves between devices by JAX's collectives and lax.ppermute only.
A program may use at most 128 MiB of HBM per device.

```python
import math
import jax
import jax.numpy as jnp
import numpy as np
from jax import lax

D = 4096
SEQS = 8
H = 256
TOKW = 512
MAXLEN = 128
WORKERS = 16


def forced_worker(key):
    return jax.random.randint(jax.random.fold_in(key, 7), (), 5, WORKERS - 5, dtype=jnp.int32)


def capped_counts(key, salt, limits):
    raw_counts = jax.random.randint(jax.random.fold_in(key, salt), (WORKERS,), 0, 6, dtype=jnp.int32)
    worker_index = jnp.arange(WORKERS, dtype=jnp.int32)
    capped = jnp.minimum(raw_counts, jnp.minimum(limits, 5))
    return jnp.where(worker_index == forced_worker(key), 5, capped).astype(jnp.int32)


def draw_count_left(key, part):
    worker_index = jnp.arange(WORKERS, dtype=jnp.int32)
    return capped_counts(key, 11, worker_index)


def draw_count_right(key, part):
    worker_index = jnp.arange(WORKERS, dtype=jnp.int32)
    return capped_counts(key, 13, WORKERS - 1 - worker_index)


def block_scale(rng, dims, pieces, smallest, top_value):
    def one(position, blocks):
        draws = jax.random.uniform(jax.random.fold_in(jax.random.fold_in(rng, 6), position), (blocks,), jnp.float32, smallest / len(pieces), top_value / len(pieces))
        return jnp.repeat(jnp.exp(draws), dims[position] // blocks).reshape((-1,) + (1,) * (len(dims) - position - 1))

    factor_of = one(*pieces[0])
    for cut in pieces[1:]:
        factor_of = factor_of * one(*cut)
    return factor_of


def length_profile(number_of, total, bound, lean):
    weights = [(1 << 20) // math.isqrt(grade ** lean) + 1 for grade in range(2, number_of + 1)]
    surplus, holding = total - bound - (number_of - 1), [1] * (number_of - 1)
    while surplus > 0:
        free = [i for i in range(number_of - 1) if holding[i] < bound]
        whole, remaining = sum([weights[i] for i in free]), surplus
        for i in free:
            extra = min(bound - holding[i], max(1, remaining * weights[i] // whole), surplus)
            holding[i] = holding[i] + extra
            surplus = surplus - extra
    return np.array([bound] + holding)


def ragged(rng, amount, total, bound, lean):
    if amount == 2:
        one = jax.random.randint(rng, (), max(1, total - bound), min(bound, total - 1) + 1)
        return jnp.stack([one, total - one])
    tallies = jnp.asarray(length_profile(amount, total, bound, lean), jnp.int32)
    couples = (amount - 1) // 2
    source_of, sink = tallies[1:1 + 2 * couples:2], tallies[2:2 + 2 * couples:2]
    margin = jnp.minimum(source_of - 1, bound - sink)
    moved = jax.random.randint(jax.random.fold_in(rng, 1), (couples,), 0, 1 << 20) % (margin + 1)
    tallies = tallies.at[1:1 + 2 * couples:2].set(source_of - moved).at[2:2 + 2 * couples:2].set(sink + moved)
    return tallies[jax.random.permutation(jax.random.fold_in(rng, 2), amount)]


def normal_values(key, dims, width, reach, split=(), kind=jnp.bfloat16):
    entries = jax.random.normal(key, dims, jnp.float32) * width
    if len(split) > 0:
        entries = block_scale(key, dims, split, -0.22, 0.18) * entries
    return jnp.clip(entries, min=-reach, max=reach).astype(kind)


def setup_inputs(seed: int = 0) -> dict:
    key_list = jax.random.split(jax.random.key(seed), 10)
    w_pair = normal_values(key_list[0], (WORKERS, 2, H, D), 1.0, 6.0, ((0, 16), (2, 2)))
    w_down = normal_values(key_list[1], (WORKERS, H, D), 1.0, 6.0, ((0, 16), (1, 2)))
    tokens = normal_values(key_list[2], (WORKERS, TOKW, D), 1.0, 6.0, ((0, 16), (1, 2)))
    cotangent = normal_values(key_list[3], (WORKERS, TOKW, D), 1.0, 6.0, ((0, 16), (1, 2)))
    seq_ids = jax.vmap(lambda own: jnp.searchsorted(jnp.cumsum(ragged(own, SEQS, TOKW, MAXLEN, 1)), jnp.arange(TOKW), side="right"))(jax.random.split(key_list[4], WORKERS)).reshape((WORKERS, TOKW)).astype(jnp.int32)
    msg_left = normal_values(key_list[5], (WORKERS, 2, H, D), 1.5, 9.0, ((0, 16), (2, 2)))
    msg_right = normal_values(key_list[6], (WORKERS, 2, H, D), 1.5, 9.0, ((0, 16), (2, 2)))
    count_left = draw_count_left(jax.random.fold_in(key_list[9], 71), 0)
    count_right = draw_count_right(jax.random.fold_in(key_list[9], 71), 0)
    return {"w_pair": w_pair, "w_down": w_down, "tokens": tokens, "cotangent": cotangent, "seq_ids": seq_ids, "msg_left": msg_left, "msg_right": msg_right, "count_left": count_left, "count_right": count_right}


learn_rate = 1.0


def worker_half(packed):
    w_pair_one, w_down_one, tokens_one, cotangent_one, seq_one = packed
    width_scale = D ** -0.5
    gate_pre = jnp.dot(tokens_one, w_pair_one[0].T, preferred_element_type=jnp.float32) * width_scale
    up_pre = jnp.dot(tokens_one, w_pair_one[1].T, preferred_element_type=jnp.float32) * width_scale
    one_hot = (seq_one[:, None] == jnp.arange(SEQS, dtype=jnp.int32)[None, :]).astype(jnp.float32)
    seq_count = jnp.sum(one_hot, axis=0)
    seq_len = jnp.sum(one_hot * seq_count[None, :], axis=1)
    tok_weight = (TOKW / SEQS) / seq_len
    scaled_cot = (tok_weight[:, None] * cotangent_one.astype(jnp.float32)).astype(jnp.bfloat16)
    grad_hidden = jnp.dot(scaled_cot, w_down_one.T, preferred_element_type=jnp.float32) * width_scale
    sigmoid_gate = jax.nn.sigmoid(gate_pre)
    grad_gate = (grad_hidden * up_pre * sigmoid_gate * (1.0 + gate_pre * (1.0 - sigmoid_gate))).astype(jnp.bfloat16)
    grad_up = (grad_hidden * gate_pre * sigmoid_gate).astype(jnp.bfloat16)
    batch_scale = TOKW ** -0.5
    gate_weight_grad = jnp.dot(grad_gate.T, tokens_one, preferred_element_type=jnp.float32) * batch_scale
    up_weight_grad = jnp.dot(grad_up.T, tokens_one, preferred_element_type=jnp.float32) * batch_scale
    return w_pair_one.astype(jnp.float32) - learn_rate * jnp.stack([gate_weight_grad, up_weight_grad])


def reference(w_pair, w_down, tokens, cotangent, seq_ids, msg_left, msg_right, count_left, count_right):
    half_step = lax.map(worker_half, (w_pair, w_down, tokens, cotangent, seq_ids))
    send_right = (half_step + msg_left.astype(jnp.float32)).astype(jnp.bfloat16)
    send_left = (half_step + msg_right.astype(jnp.float32)).astype(jnp.bfloat16)
    zero_msg = jnp.zeros_like(send_right[:1])
    recv_left = jnp.concatenate([zero_msg, send_right[:-1]], axis=0)
    recv_right = jnp.concatenate([send_left[1:], zero_msg], axis=0)
    zero_count = jnp.zeros((1,), jnp.int32)
    cnt_left = jnp.concatenate([zero_count, (count_left[:-1] + 1).astype(jnp.int32)], axis=0)
    cnt_right = jnp.concatenate([(count_right[1:] + 1).astype(jnp.int32), zero_count], axis=0)
    total_count = (1 + cnt_left + cnt_right).astype(jnp.float32)
    summed = half_step + recv_left.astype(jnp.float32) + recv_right.astype(jnp.float32)
    return (summed / total_count[:, None, None, None]).astype(jnp.bfloat16)
```

```python
import jax
import jax.numpy as jnp
from jax import lax
from jax.sharding import PartitionSpec as P


SEQS = 8
learn_rate = 1.0
CHUNKS = (1, 1, 2)

NT = (((1,), (1,)), ((), ()))
NN = (((1,), (0,)), ((), ()))


def dot(a, b, dims):
    return lax.dot_general(a, b, dims, preferred_element_type=jnp.float32)


def passed_along(shard, axis, by):
    peers = lax.axis_size(axis)
    pairs = [(i, i + by) for i in range(peers) if 0 <= i + by < peers]
    return lax.ppermute(shard, axis, pairs)


def swapped(shard):
    return lax.ppermute(shard, "shard", [(0, 1), (1, 0)])


def body(w_pair, w_down, tokens, cotangent, seq_ids, msg_left, msg_right, count_left, count_right):
    pair = w_pair[0]
    down = w_down[0]
    tok_own = tokens[0]
    ids = seq_ids[0]
    left_in, right_in = msg_left[0], msg_right[0]
    hidden, width = down.shape
    rows = tok_own.shape[0]
    total_rows = rows * lax.axis_size("shard")
    width_scale = width ** (-0.5)
    batch_scale = total_rows ** (-0.5)
    unit = hidden // sum(CHUNKS)
    bounds, at = [], 0
    for c in CHUNKS:
        bounds.append((at, at + c * unit))
        at += c * unit

    one_hot = (ids[:, None] == jnp.arange(SEQS, dtype=jnp.int32)[None, :]).astype(jnp.float32)
    own_count = jnp.sum(one_hot, axis=0)
    down_par = swapped(down[bounds[0][0] : bounds[0][1]])
    seq_count = own_count + swapped(own_count)
    tok_par = swapped(tok_own)

    cnt_left = passed_along(1 + count_left, "chain", 1)
    cnt_right = passed_along(1 + count_right, "chain", -1)
    total_count = (1 + cnt_left + cnt_right).astype(jnp.float32)

    seq_len = jnp.sum(one_hot * seq_count[None, :], axis=1)
    tok_weight = total_rows / SEQS / seq_len
    tok_weight, total_count = lax.optimization_barrier((tok_weight, total_count))
    scaled_cot = (tok_weight[:, None] * cotangent[0].astype(jnp.float32)).astype(jnp.bfloat16)

    flat_pair = pair.reshape(2 * hidden, width)
    pre_own = dot(flat_pair, tok_own, NT) * width_scale
    gh_own = dot(down, scaled_cot, NT) * width_scale
    pre_par = dot(flat_pair, tok_par, NT) * width_scale

    def grads_pre(pre, gh, lo, hi):
        gate = pre[lo:hi]
        up = pre[hidden + lo : hidden + hi]
        s = jax.nn.sigmoid(gate)
        grad_gate = (gh * up * s * (1.0 + gate * (1.0 - s))).astype(jnp.bfloat16)
        grad_up = (gh * gate * s).astype(jnp.bfloat16)
        return jnp.concatenate([grad_gate, grad_up], axis=0)

    out = jnp.zeros((1,) + pair.shape, jnp.bfloat16)
    waiting = []
    for k, (lo, hi) in enumerate(bounds):
        gh_send = dot(down_par, scaled_cot, NT) * width_scale
        gh_p = swapped(gh_send)
        if k + 1 < len(bounds):
            down_next = down[bounds[k + 1][0] : bounds[k + 1][1]]
            down_next, gh_send = lax.optimization_barrier((down_next, gh_send))
            down_par = swapped(down_next)
        g_own = grads_pre(pre_own, gh_own[lo:hi], lo, hi)
        g_par = grads_pre(pre_par, gh_p, lo, hi)
        grad = dot(g_own, tok_own, NN) + dot(g_par, tok_par, NN)
        grad = grad.reshape(2, hi - lo, width) * batch_scale
        half = pair[:, lo:hi].astype(jnp.float32) - learn_rate * grad
        send_right = (half + left_in[:, lo:hi].astype(jnp.float32)).astype(jnp.bfloat16)
        send_left = (half + right_in[:, lo:hi].astype(jnp.float32)).astype(jnp.bfloat16)
        if k + 1 < len(bounds):
            down_par, send_right, send_left = lax.optimization_barrier(
                (down_par, send_right, send_left)
            )
        recv_left = passed_along(send_right, "chain", 1)
        recv_right = passed_along(send_left, "chain", -1)
        waiting.append((lo, half, recv_left, recv_right))
    for lo, half, recv_left, recv_right in waiting:
        new = (half + recv_left.astype(jnp.float32) + recv_right.astype(jnp.float32)) / total_count
        out = lax.dynamic_update_slice(out, new.astype(jnp.bfloat16)[None], (0, 0, lo, 0))
    return out


def solution(mesh):
    return jax.shard_map(
        body,
        mesh=mesh,
        in_specs=(
            P("chain", None, "shard", None),
            P("chain", "shard", None),
            P("chain", "shard", None),
            P("chain", "shard", None),
            P("chain", "shard"),
            P("chain", None, "shard", None),
            P("chain", None, "shard", None),
            P("chain"),
            P("chain"),
        ),
        out_specs=P("chain", None, "shard", None),
        check_vma=False,
    )
```

```python
import jax
import jax.numpy as jnp
from jax import lax
from jax.sharding import PartitionSpec as P


SEQS = 8
learn_rate = 1.0
CHUNKS = (1, 1, 1, 1)

NT = (((1,), (1,)), ((), ()))
NN = (((1,), (0,)), ((), ()))


def dot(a, b, dims):
    return lax.dot_general(a, b, dims, preferred_element_type=jnp.float32)


def paired(shard, first):
    peers = lax.axis_size("chain")
    lows = range(first, peers - 1, 2)
    return lax.ppermute(shard, "chain", [p for i in lows for p in ((i, i + 1), (i + 1, i))])


def swapped(shard):
    return lax.ppermute(shard, "shard", [(0, 1), (1, 0)])


def body(w_pair, w_down, tokens, cotangent, seq_ids, msg_left, msg_right, count_left, count_right):
    pair = w_pair[0]
    down = w_down[0]
    tok_own = tokens[0]
    ids = seq_ids[0]
    left_in, right_in = msg_left[0], msg_right[0]
    hidden, width = down.shape
    rows = tok_own.shape[0]
    total_rows = rows * lax.axis_size("shard")
    width_scale = width ** (-0.5)
    batch_scale = total_rows ** (-0.5)
    unit = hidden // sum(CHUNKS)
    bounds, at = [], 0
    for c in CHUNKS:
        bounds.append((at, at + c * unit))
        at += c * unit

    one_hot = (ids[:, None] == jnp.arange(SEQS, dtype=jnp.int32)[None, :]).astype(jnp.float32)
    own_count = jnp.sum(one_hot, axis=0)
    down_par = swapped(down[bounds[0][0] : bounds[0][1]])
    seq_count = own_count + swapped(own_count)
    cut = rows // 2
    tok_a = swapped(tok_own[:cut])
    tok_b = swapped(tok_own[cut:])

    odd = lax.axis_index("chain") % 2 == 1
    count_far = 1 + jnp.where(odd, count_left, count_right)
    count_near = 1 + jnp.where(odd, count_right, count_left)
    cnt_far = paired(count_far, 1)
    cnt_near = paired(count_near, 0)
    total_count = (1 + cnt_far + cnt_near).astype(jnp.float32)
    pair_f32 = pair.astype(jnp.float32)
    base_far = pair_f32 + jnp.where(odd, left_in, right_in).astype(jnp.float32)
    base_near = pair_f32 + jnp.where(odd, right_in, left_in).astype(jnp.float32)

    seq_len = jnp.sum(one_hot * seq_count[None, :], axis=1)
    tok_weight = total_rows / SEQS / seq_len
    tok_weight, total_count, base_far, base_near = lax.optimization_barrier(
        (tok_weight, total_count, base_far, base_near)
    )
    scaled_cot = (tok_weight[:, None] * cotangent[0].astype(jnp.float32)).astype(jnp.bfloat16)

    flat_pair = pair.reshape(2 * hidden, width)
    pre_own = dot(flat_pair, tok_own, NT) * width_scale
    gh_own = dot(down, scaled_cot, NT) * width_scale
    pre_par = jnp.concatenate([dot(flat_pair, t, NT) for t in (tok_a, tok_b)], 1) * width_scale

    def grads_pre(pre, gh, lo, hi):
        gate = pre[lo:hi]
        up = pre[hidden + lo : hidden + hi]
        s = jax.nn.sigmoid(gate)
        grad_gate = (gh * up * s * (1.0 + gate * (1.0 - s))).astype(jnp.bfloat16)
        grad_up = (gh * gate * s).astype(jnp.bfloat16)
        return jnp.concatenate([grad_gate, grad_up], axis=0)

    out = jnp.zeros((1,) + pair.shape, jnp.bfloat16)
    waiting = []
    for k, (lo, hi) in enumerate(bounds):
        gh_send = dot(down_par, scaled_cot, NT) * width_scale
        gh_p = swapped(gh_send)
        if k + 1 < len(bounds):
            down_next = down[bounds[k + 1][0] : bounds[k + 1][1]]
            down_next, gh_send = lax.optimization_barrier((down_next, gh_send))
            down_par = swapped(down_next)
        g_own = grads_pre(pre_own, gh_own[lo:hi], lo, hi)
        g_par = grads_pre(pre_par, gh_p, lo, hi)
        grad = (
            dot(g_own, tok_own, NN)
            + dot(g_par[:, :cut], tok_a, NN)
            + dot(g_par[:, cut:], tok_b, NN)
        )
        step = learn_rate * (grad.reshape(2, hi - lo, width) * batch_scale)
        send_far = (base_far[:, lo:hi] - step).astype(jnp.bfloat16)
        send_near = (base_near[:, lo:hi] - step).astype(jnp.bfloat16)
        if k + 1 < len(bounds):
            down_par, _, _ = lax.optimization_barrier((down_par, send_far, send_near))
        recv_far = paired(send_far, 1)
        recv_near = paired(send_near, 0)
        half = pair[:, lo:hi].astype(jnp.float32) - step
        waiting.append((lo, half, recv_far, recv_near))
    for lo, half, recv_far, recv_near in waiting:
        new = (half + recv_far.astype(jnp.float32) + recv_near.astype(jnp.float32)) / total_count
        out = lax.dynamic_update_slice(out, new.astype(jnp.bfloat16)[None], (0, 0, lo, 0))
    return out


def solution(mesh):
    return jax.shard_map(
        body,
        mesh=mesh,
        in_specs=(
            P("chain", None, "shard", None),
            P("chain", "shard", None),
            P("chain", "shard", None),
            P("chain", "shard", None),
            P("chain", "shard"),
            P("chain", None, "shard", None),
            P("chain", None, "shard", None),
            P("chain"),
            P("chain"),
        ),
        out_specs=P("chain", None, "shard", None),
        check_vma=False,
    )
```

```python
import jax
import jax.numpy as jnp
from jax import lax
from jax.sharding import PartitionSpec as P


SEQS = 8
learn_rate = 1.0
CHUNKS = (1, 1, 1, 1)
REMADE = 5

NT = (((1,), (1,)), ((), ()))
NN = (((1,), (0,)), ((), ()))


def dot(a, b, dims):
    return lax.dot_general(a, b, dims, preferred_element_type=jnp.float32)


def paired(shard, first):
    peers = lax.axis_size("chain")
    lows = range(first, peers - 1, 2)
    return lax.ppermute(shard, "chain", [p for i in lows for p in ((i, i + 1), (i + 1, i))])


def swapped(shard):
    return lax.ppermute(shard, "shard", [(0, 1), (1, 0)])


def body(w_pair, w_down, tokens, cotangent, seq_ids, msg_left, msg_right, count_left, count_right):
    pair = w_pair[0]
    down = w_down[0]
    tok_own = tokens[0]
    ids = seq_ids[0]
    left_in, right_in = msg_left[0], msg_right[0]
    hidden, width = down.shape
    rows = tok_own.shape[0]
    total_rows = rows * lax.axis_size("shard")
    width_scale = width ** (-0.5)
    batch_scale = total_rows ** (-0.5)
    unit = hidden // sum(CHUNKS)
    bounds, at = [], 0
    for c in CHUNKS:
        bounds.append((at, at + c * unit))
        at += c * unit

    one_hot = (ids[:, None] == jnp.arange(SEQS, dtype=jnp.int32)[None, :]).astype(jnp.float32)
    own_count = jnp.sum(one_hot, axis=0)
    down_par = swapped(down[bounds[0][0] : bounds[0][1]])
    seq_count = own_count + swapped(own_count)
    cut = width * REMADE // 16
    tok_a = swapped(tok_own[:, :cut])
    tok_b = swapped(tok_own[:, cut:])

    odd = lax.axis_index("chain") % 2 == 1
    count_far = 1 + jnp.where(odd, count_left, count_right)
    count_near = 1 + jnp.where(odd, count_right, count_left)
    cnt_far = paired(count_far, 1)
    cnt_near = paired(count_near, 0)
    total_count = (1 + cnt_far + cnt_near).astype(jnp.float32)
    pair_f32 = pair.astype(jnp.float32)
    base_far = pair_f32 + jnp.where(odd, left_in, right_in).astype(jnp.float32)
    base_near = pair_f32 + jnp.where(odd, right_in, left_in).astype(jnp.float32)
    far_tok_own = paired(tok_own[:, :cut], 1)
    far_base = paired(base_far[:, :, :cut].astype(jnp.bfloat16), 1)
    far_tok_par = paired(tok_a, 1)

    seq_len = jnp.sum(one_hot * seq_count[None, :], axis=1)
    tok_weight = total_rows / SEQS / seq_len
    scaled_cot = (tok_weight[:, None] * cotangent[0].astype(jnp.float32)).astype(jnp.bfloat16)

    flat_pair = pair.reshape(2 * hidden, width)
    pre_own = dot(flat_pair, tok_own, NT) * width_scale
    gh_own = dot(down, scaled_cot, NT) * width_scale
    pre_par = (
        dot(flat_pair[:, :cut], tok_a, NT) + dot(flat_pair[:, cut:], tok_b, NT)
    ) * width_scale

    def grads_pre(pre, gh, lo, hi):
        gate = pre[lo:hi]
        up = pre[hidden + lo : hidden + hi]
        s = jax.nn.sigmoid(gate)
        grad_gate = (gh * up * s * (1.0 + gate * (1.0 - s))).astype(jnp.bfloat16)
        grad_up = (gh * gate * s).astype(jnp.bfloat16)
        return jnp.concatenate([grad_gate, grad_up], axis=0)

    def step_of(grad, chunk):
        return learn_rate * (grad.reshape(2, chunk, grad.shape[1]) * batch_scale)

    out = jnp.zeros((1,) + pair.shape, jnp.bfloat16)
    waiting = []
    ends = [down[lo:hi] for lo, hi in bounds]
    down_par = {0: down_par}
    for k, (lo, hi) in enumerate(bounds):
        gh_send = dot(down_par[k], scaled_cot, NT) * width_scale
        gh_p = swapped(gh_send)
        if k == 0:
            for j in range(1, len(bounds)):
                down_par[j] = swapped(ends[j])
        g_own = grads_pre(pre_own, gh_own[lo:hi], lo, hi)
        g_par = grads_pre(pre_par, gh_p, lo, hi)
        step_a = step_of(
            dot(g_own, tok_own[:, :cut], NN) + dot(g_par, tok_a, NN), hi - lo
        )
        step_b = step_of(
            dot(g_own, tok_own[:, cut:], NN) + dot(g_par, tok_b, NN), hi - lo
        )
        send_far = (base_far[:, lo:hi, cut:] - step_b).astype(jnp.bfloat16)
        grads = jnp.concatenate([g_own, g_par], axis=1).reshape(2, hi - lo, total_rows)
        send_far = jnp.concatenate([send_far, grads], axis=2)
        send_near = jnp.concatenate(
            [
                (base_near[:, lo:hi, :cut] - step_a).astype(jnp.bfloat16),
                (base_near[:, lo:hi, cut:] - step_b).astype(jnp.bfloat16),
            ],
            axis=2,
        )
        if k + 1 < len(bounds):
            base_near, base_far, _, _, down_par[k + 1] = lax.optimization_barrier(
                (base_near, base_far, send_near, send_far, down_par[k + 1])
            )
        recv_far = paired(send_far, 1)
        recv_near = paired(send_near, 0)
        half_a = pair[:, lo:hi, :cut].astype(jnp.float32) - step_a
        half_b = pair[:, lo:hi, cut:].astype(jnp.float32) - step_b
        waiting.append((lo, hi, half_a, half_b, recv_far, recv_near))
    for k, (lo, hi, half_a, half_b, recv_far, recv_near) in enumerate(waiting):
        if k > 0:
            recv_far, recv_near, out = lax.optimization_barrier((recv_far, recv_near, out))
        far_grads = recv_far[:, :, width - cut :].reshape(2 * (hi - lo), total_rows)
        far_step = step_of(
            dot(far_grads[:, :rows], far_tok_own, NN)
            + dot(far_grads[:, rows:], far_tok_par, NN),
            hi - lo,
        )
        far_a = (far_base[:, lo:hi].astype(jnp.float32) - far_step).astype(jnp.bfloat16)
        far_b = recv_far[:, :, : width - cut]
        near_a, near_b = recv_near[:, :, :cut], recv_near[:, :, cut:]
        for at, half, far, near in ((cut, half_b, far_b, near_b), (0, half_a, far_a, near_a)):
            new = (half + far.astype(jnp.float32) + near.astype(jnp.float32)) / total_count
            out = lax.dynamic_update_slice(out, new.astype(jnp.bfloat16)[None], (0, 0, lo, at))
    return out


def solution(mesh):
    return jax.shard_map(
        body,
        mesh=mesh,
        in_specs=(
            P("chain", None, "shard", None),
            P("chain", "shard", None),
            P("chain", "shard", None),
            P("chain", "shard", None),
            P("chain", "shard"),
            P("chain", None, "shard", None),
            P("chain", None, "shard", None),
            P("chain"),
            P("chain"),
        ),
        out_specs=P("chain", None, "shard", None),
        check_vma=False,
    )
```
